32 devices in a mesh: group: 4 (over y, x), expert: 4 (over z), dp: 2 (over core).
Axes of the slice: x: 2, y: 2, z: 4, core: 2. Of those that a mesh axis runs over, the one named last changes fastest.
Arguments:
- tokens: bfloat16 [8, 16, 7168], P(('expert', 'dp'), 'group'), may hold values from -6 to 6
- expert_ids: int32 [8, 16, 8], P(('expert', 'dp')), may hold values from 0 to 31, as said below
- gate_codes: int32 [8, 16, 8], P(('expert', 'dp')), may hold values from 1 to 1023
- w_gate: bfloat16 [4, 7168, 2048], P('expert', None, 'group'), may hold values from -0.0625 to 0.0625
- w_up: bfloat16 [4, 7168, 2048], P('expert', None, 'group'), may hold values from -0.0625 to 0.0625
- w_down: bfloat16 [4, 2048, 7168], P('expert', 'group'), may hold values from -0.125 to 0.125
Outputs:
- mixed: bfloat16 [8, 16, 7168], P(('expert', 'dp'), 'group')
The draws below stay inside these ranges and needn't reach their ends.
Inputs may be any that keep to these rules, and one draw needn't show every extreme that they name: `expert_ids`: each token names 8 different experts, all within at most 4 of the 8 groups of 4 consecutive ids. In every set (one index of the first dimension), each expert below 4 is named by at most 4 tokens, and some expert by exactly 4; a token names at most 4 experts below 4.
All inputs are finite; a program needn't handle non-finite values.
Results may differ from the reference program's by a relative error of at most 0.015.
Values may be sent and summed in bfloat16 or wider, within the bound.
A program may use at most 64 MiB of HBM per device.

```python
import jax
import jax.numpy as jnp
from jax import lax

D = 7168
FF = 2048
TOP = 8
NODE_GROUPS = 8
MAX_NODES = 4
CAPG = 4
EXPERTS = 4
SET_TOK = 16
SETS = 8
N_GROUP = 4


def draw_others(key, count):
    keys = jax.random.split(key, 3)
    groups = jax.random.permutation(keys[0], NODE_GROUPS - 1)[:MAX_NODES] + 1
    fewer = jax.random.permutation(keys[1], (MAX_NODES - 1) * EXPERTS)[:TOP]
    wider = jax.random.permutation(keys[2], MAX_NODES * EXPERTS)[:TOP]
    local = jnp.where(count > 0, fewer, wider)
    return groups[local // EXPERTS] * EXPERTS + local % EXPERTS


def shuffle_row(key, row):
    return jax.random.permutation(key, row)


def draw_one_set(key):
    keys = jax.random.split(key, 6)
    spacing = SET_TOK // CAPG
    offsets = jax.random.permutation(keys[0], SET_TOK)[:EXPERTS]
    order = jax.random.permutation(keys[1], SET_TOK)
    slot_index = jnp.arange(CAPG)
    slot_token = order[(offsets[:, None] + spacing * slot_index[None, :]) % SET_TOK]
    live = jax.random.randint(keys[2], (EXPERTS, CAPG), 0, 2)
    chosen = jax.random.randint(keys[3], (), 0, EXPERTS)
    live = jnp.where(jnp.arange(EXPERTS)[:, None] == chosen, 1, live)
    token_index = jnp.arange(SET_TOK)
    member = jnp.sum(jnp.where(slot_token[None, :, :] == token_index[:, None, None], live[None, :, :], 0), axis=2)
    count = jnp.sum(member, axis=1)
    position = jnp.cumsum(member, axis=1) - member
    picks = jnp.arange(TOP)
    window_ids = jnp.sum(jnp.where((member[:, :, None] == 1) & (position[:, :, None] == picks[None, None, :]), jnp.arange(EXPERTS)[None, :, None], 0), axis=1)
    others = jax.vmap(draw_others)(jax.random.split(keys[4], SET_TOK), count)
    offset_pick = jnp.clip(picks[None, :] - count[:, None], 0, TOP - 1)
    other_ids = jnp.take_along_axis(others, offset_pick, axis=1)
    chosen_ids = jnp.where(picks[None, :] < count[:, None], window_ids, other_ids)
    return jax.vmap(shuffle_row)(jax.random.split(keys[5], SET_TOK), chosen_ids)


def draw_expert_ids(key, part):
    keys = jax.random.split(jax.random.fold_in(key, 17), SETS)
    return jax.vmap(draw_one_set)(keys).astype(jnp.int32)


def with_ends(array, key, low, high):
    index_at = [jax.random.randint(jax.random.fold_in(key, axis), (), 0, length) for axis, length in enumerate(array.shape)]
    longest = array.shape.index(max(array.shape))
    beside = index_at[:longest] + [(index_at[longest] + 1) % array.shape[longest]] + index_at[longest + 1:]
    return array.at[tuple(index_at)].set(low).at[tuple(beside)].set(high)


def block_levels(key, shape, pieces, smallest, largest):
    def one(axis_at, blocks):
        steps = jax.random.uniform(jax.random.fold_in(jax.random.fold_in(key, 6), axis_at), (blocks,), jnp.float32, smallest / len(pieces), largest / len(pieces))
        return jnp.repeat(jnp.exp(steps), shape[axis_at] // blocks).reshape((-1,) + (1,) * (len(shape) - axis_at - 1))

    level = one(*pieces[0])
    for cut in pieces[1:]:
        level = level * one(*cut)
    return level


def noise(rng, dims, deviation, bound, shards=(), kind=jnp.bfloat16):
    array = deviation * jax.random.normal(rng, dims, jnp.float32)
    if shards:
        array = array * block_levels(rng, dims, shards, -0.22, 0.18)
    return jnp.clip(array, -bound, bound).astype(kind)


def setup_inputs(seed: int = 0) -> dict:
    key_of = jax.random.split(jax.random.key(seed), 7)
    return {
        "tokens": noise(key_of[0], (SETS, SET_TOK, D), 1.0, 6.0, ((0, 8), (1, 4))),
        "expert_ids": draw_expert_ids(jax.random.fold_in(key_of[6], 71), 0),
        "gate_codes": with_ends(jax.random.randint(key_of[2], (SETS, SET_TOK, TOP), 1, 1024), jax.random.fold_in(key_of[2], 1), 1, 1023).astype(jnp.int32),
        "w_gate": noise(key_of[3], (EXPERTS, D, FF), D ** -0.5, 0.0625, ((0, 4), (2, 4))),
        "w_up": noise(key_of[4], (EXPERTS, D, FF), D ** -0.5, 0.0625, ((0, 4), (2, 4))),
        "w_down": noise(key_of[5], (EXPERTS, FF, D), FF ** -0.5, 0.125, ((0, 4), (1, 4))),
    }


def routing(expert_ids, gate_codes):
    codes = gate_codes.astype(jnp.float32)
    gates = 2.5 * codes / jnp.sum(codes, axis=-1, keepdims=True)
    window = jnp.arange(EXPERTS, dtype=jnp.int32)
    hits = expert_ids[..., None] == window
    member = jnp.any(hits, axis=-2).astype(jnp.int32)
    weight = jnp.sum(jnp.where(hits, gates[..., None], jnp.float32(0.0)), axis=-2)
    rank = jnp.cumsum(member, axis=-2) - member
    slots = jnp.arange(CAPG, dtype=jnp.int32)
    place = (member[..., None] == 1) & (rank[..., None] == slots)
    return place, weight


def reference(tokens, expert_ids, gate_codes, w_gate, w_up, w_down):
    place, weight = routing(expert_ids, gate_codes)
    pick = place.astype(jnp.float32)
    rows = jnp.einsum("stej,std->sejd", pick, tokens.astype(jnp.float32)).astype(jnp.bfloat16)
    slices = N_GROUP
    hid_dev = FF // slices

    def one_expert(items):
        expert_rows, gate_mat, up_mat, down_mat = items
        flat = expert_rows.reshape(SETS * CAPG, D)
        first = jnp.dot(flat, gate_mat, preferred_element_type=jnp.float32)
        second = jnp.dot(flat, up_mat, preferred_element_type=jnp.float32)
        hidden = (jax.nn.silu(first) * second).astype(jnp.bfloat16)
        parts = jnp.einsum("rgh,ghd->grd", hidden.reshape(SETS * CAPG, slices, hid_dev).astype(jnp.float32),
                           down_mat.reshape(slices, hid_dev, D).astype(jnp.float32))
        parts = lax.optimization_barrier(parts.astype(jnp.bfloat16)).astype(jnp.float32)
        return jnp.sum(parts, axis=0).reshape(SETS, CAPG, D)

    outs = lax.map(one_expert, (jnp.transpose(rows, (1, 0, 2, 3)), w_gate, w_up, w_down))
    mix = jnp.where(place, weight[..., None], jnp.float32(0.0))
    mixed = jnp.einsum("stej,esjd->std", mix, outs, precision=lax.Precision.HIGHEST)
    return mixed.astype(jnp.bfloat16)
```

```python
import functools

import jax
import jax.numpy as jnp
from jax import lax
from jax.experimental import pallas as pl
from jax.experimental.pallas import tpu as pltpu
from jax.sharding import PartitionSpec as P

CAPG = 4
FORWARD = (1, 1, 1, 1)
BACK = (1, 1, 1, 1)
MESH = pl.DeviceIdType.MESH


def dot(a, b):
    return jnp.dot(a, b, preferred_element_type=jnp.float32)


def routing(ids, codes, experts, capacity):
    tokens = ids.shape[1]
    wide = experts * capacity
    codes = codes.astype(jnp.float32)
    gates = 2.5 * codes / jnp.sum(codes, axis=0, keepdims=True)
    slot = lax.broadcasted_iota(jnp.int32, (wide, tokens), 0)
    member = jnp.zeros((wide, tokens), jnp.float32)
    weight = jnp.zeros((wide, tokens), jnp.float32)
    for e in range(experts):
        hits = ids == e
        named = jnp.max(jnp.where(hits, 1.0, 0.0), axis=0, keepdims=True)
        gate = jnp.sum(jnp.where(hits, gates, 0.0), axis=0, keepdims=True)
        mine = (slot >= e * capacity) & (slot < (e + 1) * capacity)
        member = jnp.where(mine, named, member)
        weight = jnp.where(mine, gate, weight)
    row = lax.broadcasted_iota(jnp.int32, (tokens, tokens), 0)
    column = lax.broadcasted_iota(jnp.int32, (tokens, tokens), 1)
    before = jnp.where(row < column, 1.0, 0.0).astype(jnp.bfloat16)
    rank = dot(member.astype(jnp.bfloat16), before)
    place = jnp.where(rank == (slot % capacity).astype(jnp.float32), member, 0.0)
    mix = place * weight
    high = mix.astype(jnp.bfloat16)
    low = (mix - high.astype(jnp.float32)).astype(jnp.bfloat16)
    return place.astype(jnp.bfloat16), jnp.concatenate([flipped(high), flipped(low)], axis=0)


def flipped(a):
    n = a.shape[1]
    row = lax.broadcasted_iota(jnp.int32, (n, n), 0)
    column = lax.broadcasted_iota(jnp.int32, (n, n), 1)
    eye = jnp.where(row == column, 1.0, 0.0).astype(jnp.bfloat16)
    return lax.dot_general(
        eye, a, (((1,), (1,)), ((), ())), preferred_element_type=jnp.float32
    ).astype(jnp.bfloat16)


def pieces(width, shares):
    ends = [0]
    for k in range(len(shares)):
        ends.append(width * sum(shares[: k + 1]) // sum(shares) // 128 * 128)
    return [pl.ds(a, b - a) for a, b in zip(ends[:-1], ends[1:])]


def partner(a, m, n):
    out, bit = 0, 1
    while bit < n:
        out = out + bit * lax.rem(lax.div(a, bit) + m // bit % 2, 2)
        bit *= 2
    return out


def kernel(
    groups, experts, sets, tokens, ids, codes, w_gate, w_up, w_down, red,
    tok, named, wgu, wd, rows, slots, acc, part, ret, mixed,
    tok_sem, in_sem, w_sem, d_sem, id_s, id_r, ga_s, ga_r, di_s, di_r, re_s, re_r, sc_s, sc_r, go,
):
    g = lax.axis_index("group")
    z = lax.axis_index("expert")
    d = lax.axis_index("dp")
    lead = sets - 1
    own, width = tokens.shape
    cuts = pieces(width, FORWARD)
    back_cuts = pieces(width, BACK)
    cap = CAPG
    peer = [partner(g, m, groups) for m in range(groups)]
    far = [partner(z, m, experts) for m in range(experts)]
    group_order = list(range(groups - 1, -1, -1))
    expert_order = list(range(experts - 1, -1, -1))
    barrier = pltpu.get_barrier_semaphore()

    tok_in = pltpu.make_async_copy(tokens, tok.at[d, g], tok_sem)
    tok_in.start()
    pltpu.make_async_copy(ids, named.at[d, 0], in_sem).start()
    pltpu.make_async_copy(codes, named.at[d, 1], in_sem).start()
    named_in = pltpu.make_async_copy(named.at[d], named.at[d], in_sem)

    def greet(**to):
        pl.semaphore_signal(barrier, inc=1, device_id=to, device_id_type=MESH)

    def remote(to, src, dst, send, recv):
        return pltpu.make_async_remote_copy(
            src_ref=src, dst_ref=dst, send_sem=send, recv_sem=recv,
            device_id=to, device_id_type=MESH,
        )

    def landed(ref, sem):
        pltpu.make_async_copy(ref, ref, sem).wait()

    def load():
        for c, cut in enumerate(cuts):
            pltpu.make_async_copy(w_gate.at[cut, :], wgu.at[0, cut, :], w_sem.at[c]).start()
            pltpu.make_async_copy(w_up.at[cut, :], wgu.at[1, cut, :], w_sem.at[c]).start()
        for c, cut in enumerate(back_cuts):
            pltpu.make_async_copy(w_down.at[:, cut], wd.at[:, cut], d_sem.at[c]).start()

    def send_tokens(order):
        for cut, sem in zip(cuts, range(len(cuts))):
            for m in order:
                remote(
                    {"group": peer[m], "dp": lead}, tok.at[d, g, :, cut], tok.at[d, g, :, cut],
                    ga_s, ga_r.at[sem, d],
                ).start()

    def compute(present, order):
        for c, cut in enumerate(cuts):
            landed(slots.at[pl.ds(0, present), :, cut], di_r.at[c])
            landed(wgu.at[:, cut, :], w_sem.at[c])
            flat = slots[:, :, cut].reshape(experts * cap, cut.size)
            for i in range(2):
                made = dot(flat, wgu[i, cut, :])
                acc[i] = made if c == 0 else acc[i] + made
        hidden = (acc[0] / (1.0 + jnp.exp(-acc[0])) * acc[1]).astype(jnp.bfloat16)
        for c, cut in enumerate(back_cuts):
            landed(wd.at[:, cut], d_sem.at[c])
            made = dot(hidden, wd[:, cut]).astype(jnp.bfloat16)
            part[:, :, cut] = made.reshape(experts, cap, cut.size)
            for m in order:
                remote(
                    {"expert": far[m], "dp": lead}, part.at[far[m], :, cut], ret.at[d, z, :, cut],
                    re_s, re_r.at[c, d],
                ).start()
            if present < experts:
                ret[lead, z, :, cut] = part[z, :, cut]

    @pl.when(d == lead)
    def _():
        for m in range(1, groups):
            greet(group=peer[m])
        for m in range(1, experts):
            for s in range(lead):
                greet(expert=far[m], dp=s)
        load()
        tok_in.wait()
        pl.semaphore_wait(barrier, groups - 1 + lead)
        for s in range(lead):
            pl.semaphore_signal(go, inc=1, device_id={"dp": s}, device_id_type=MESH)
        send_tokens(group_order[:-1])

        named_in.wait()
        routes = {lead: routing(named[lead, 0], named[lead, 1], experts, cap)}
        for s in range(lead):
            landed(named.at[s], id_r.at[s])
            routes[s] = routing(named[s, 0], named[s, 1], experts, cap)

        for s in range(lead, -1, -1):
            for c, cut in enumerate(cuts):
                landed(tok.at[s, pl.ds(0, groups - 1 if s == lead else groups), :, cut], ga_r.at[c, s])
                chosen = dot(routes[s][0], tok[s, :, :, cut].reshape(groups * own, cut.size))
                rows[s, :, :, cut] = chosen.astype(jnp.bfloat16).reshape(experts, cap, cut.size)
                if (s, c) == (lead, 0):
                    pl.semaphore_wait(go, lead)
                for m in expert_order:
                    if (s, m) != (lead, 0):
                        remote(
                            {"expert": far[m], "dp": s}, rows.at[s, far[m], :, cut], slots.at[z, :, cut],
                            di_s.at[s], di_r.at[c],
                        ).start()
                if s == lead:
                    slots[z, :, cut] = rows[s, z, :, cut]

        compute(experts - 1, expert_order[:-1])

        for s in range(lead, -1, -1):
            for c, cut in enumerate(back_cuts):
                landed(ret.at[s, pl.ds(0, experts - 1 if s == lead else experts), :, cut], re_r.at[c, s])
                both = dot(routes[s][1], ret[s, :, :, cut].reshape(experts * cap, cut.size))
                total = (both[: groups * own] + both[groups * own :]).astype(jnp.bfloat16)
                mixed[s, :, :, cut] = total.reshape(groups, own, cut.size)
                for m in group_order:
                    if (s, m) != (lead, 0):
                        remote(
                            {"group": peer[m], "dp": s}, mixed.at[s, peer[m], :, cut], red.at[g, :, cut],
                            sc_s.at[s], sc_r.at[c],
                        ).start()
                if s == lead:
                    pltpu.make_async_copy(mixed.at[s, g, :, cut], red.at[g, :, cut], sc_r.at[c]).start()

        landed(tok.at[lead, pl.ds(0, groups - 1)], ga_s)
        landed(part.at[pl.ds(0, experts - 1)], re_s)
        for s in range(sets):
            landed(rows.at[s, pl.ds(0, experts - 1 if s == lead else experts)], di_s.at[s])
            landed(mixed.at[s, pl.ds(0, groups - 1 if s == lead else groups)], sc_s.at[s])

    @pl.when(d != lead)
    def _():
        greet(dp=lead)
        for m in range(1, experts):
            greet(expert=far[m])
        load()
        tok_in.wait()
        named_in.wait()
        pl.semaphore_wait(go, 1)
        send_tokens(group_order)
        remote({"dp": lead}, named.at[d], named.at[d], id_s, id_r.at[d]).start()
        pl.semaphore_wait(barrier, 2 * (experts - 1))
        pl.semaphore_signal(go, inc=1, device_id={"dp": lead}, device_id_type=MESH)

        compute(experts, expert_order)

        landed(tok.at[d], ga_s)
        landed(named.at[d], id_s)
        landed(part, re_s)

    for c, cut in enumerate(back_cuts):
        landed(red.at[:, :, cut], sc_r.at[c])


def per_device(tokens, expert_ids, gate_codes, w_gate, w_up, w_down):
    groups = lax.axis_size("group")
    experts = lax.axis_size("expert")
    sets = lax.axis_size("dp")
    own, width = tokens.shape[1:]
    hid = w_gate.shape[2]
    bf16 = jnp.bfloat16
    any_space = pl.BlockSpec(memory_space=pl.ANY)
    dma = pltpu.SemaphoreType.DMA
    shares = pl.pallas_call(
        functools.partial(kernel, groups, experts, sets),
        out_shape=jax.ShapeDtypeStruct((groups, own, width), bf16),
        in_specs=[any_space] * 6,
        out_specs=any_space,
        scratch_shapes=[
            pltpu.VMEM((sets, groups, own, width), bf16),
            pltpu.VMEM((sets, 2, *expert_ids.shape[:0:-1]), jnp.int32),
            pltpu.VMEM((2, width, hid), bf16),
            pltpu.VMEM((hid, width), bf16),
            pltpu.VMEM((sets, experts, CAPG, width), bf16),
            pltpu.VMEM((experts, CAPG, width), bf16),
            pltpu.VMEM((2, experts * CAPG, hid), jnp.float32),
            pltpu.VMEM((experts, CAPG, width), bf16),
            pltpu.VMEM((sets, experts, CAPG, width), bf16),
            pltpu.VMEM((sets, groups, own, width), bf16),
            dma,
            dma,
            dma((len(FORWARD),)),
            dma((len(BACK),)),
            dma,
            dma((sets - 1,)),
            dma,
            dma((len(FORWARD), sets)),
            dma((sets,)),
            dma((len(FORWARD),)),
            dma,
            dma((len(BACK), sets)),
            dma((sets,)),
            dma((len(BACK),)),
            pltpu.SemaphoreType.REGULAR,
        ],
        compiler_params=pltpu.CompilerParams(
            collective_id=0, has_side_effects=True, vmem_limit_bytes=60 * 1024 * 1024
        ),
    )(tokens[0], expert_ids[0].T, gate_codes[0].T, w_gate[0], w_up[0], w_down[0])
    total = shares[0].astype(jnp.float32)
    for k in range(1, groups):
        total = total + shares[k].astype(jnp.float32)
    return total.astype(bf16)[None]


def solution(mesh):
    placed = (
        P(("expert", "dp"), "group", None),
        P(("expert", "dp"), None, None),
        P(("expert", "dp"), None, None),
        P("expert", None, "group"),
        P("expert", None, "group"),
        P("expert", "group", None),
    )
    return jax.shard_map(
        per_device,
        mesh=mesh,
        in_specs=placed,
        out_specs=P(("expert", "dp"), "group", None),
        check_vma=False,
    )
```

```python
import functools

import jax
import jax.numpy as jnp
from jax import lax
from jax.experimental import pallas as pl
from jax.experimental.pallas import tpu as pltpu
from jax.sharding import PartitionSpec as P

CAPG = 4
FORWARD = (1, 2, 2, 2)
BACK = (1, 2, 2, 2)
URGENT = 1
MESH = pl.DeviceIdType.MESH


def dot(a, b):
    return jnp.dot(a, b, preferred_element_type=jnp.float32)


def routing(ids, codes, experts, capacity):
    tokens = ids.shape[1]
    wide = experts * capacity
    codes = codes.astype(jnp.float32)
    gates = 2.5 * codes / jnp.sum(codes, axis=0, keepdims=True)
    slot = lax.broadcasted_iota(jnp.int32, (wide, tokens), 0)
    member = jnp.zeros((wide, tokens), jnp.float32)
    weight = jnp.zeros((wide, tokens), jnp.float32)
    for e in range(experts):
        hits = ids == e
        named = jnp.max(jnp.where(hits, 1.0, 0.0), axis=0, keepdims=True)
        gate = jnp.sum(jnp.where(hits, gates, 0.0), axis=0, keepdims=True)
        mine = (slot >= e * capacity) & (slot < (e + 1) * capacity)
        member = jnp.where(mine, named, member)
        weight = jnp.where(mine, gate, weight)
    row = lax.broadcasted_iota(jnp.int32, (tokens, tokens), 0)
    column = lax.broadcasted_iota(jnp.int32, (tokens, tokens), 1)
    before = jnp.where(row < column, 1.0, 0.0).astype(jnp.bfloat16)
    rank = dot(member.astype(jnp.bfloat16), before)
    place = jnp.where(rank == (slot % capacity).astype(jnp.float32), member, 0.0)
    mix = place * weight
    high = mix.astype(jnp.bfloat16)
    low = (mix - high.astype(jnp.float32)).astype(jnp.bfloat16)
    return place.astype(jnp.bfloat16), jnp.concatenate([flipped(high), flipped(low)], axis=0)


def flipped(a):
    n = a.shape[1]
    row = lax.broadcasted_iota(jnp.int32, (n, n), 0)
    column = lax.broadcasted_iota(jnp.int32, (n, n), 1)
    eye = jnp.where(row == column, 1.0, 0.0).astype(jnp.bfloat16)
    return lax.dot_general(
        eye, a, (((1,), (1,)), ((), ())), preferred_element_type=jnp.float32
    ).astype(jnp.bfloat16)


def pieces(width, shares):
    ends = [0]
    for k in range(len(shares)):
        ends.append(width * sum(shares[: k + 1]) // sum(shares) // 128 * 128)
    return [pl.ds(a, b - a) for a, b in zip(ends[:-1], ends[1:])]


def partner(a, m, n):
    out, bit = 0, 1
    while bit < n:
        out = out + bit * lax.rem(lax.div(a, bit) + m // bit % 2, 2)
        bit *= 2
    return out


def ends_first(z, k, n):
    at = jnp.where(z == 0, 0, jnp.where(z == n - 1, 1, z + 1))
    i = k + jnp.where(k >= at, 1, 0)
    return jnp.where(i == 0, 0, jnp.where(i == 1, n - 1, i - 1))


def kernel(
    groups, experts, sets, tokens, ids, codes, w_gate, w_up, w_down, red,
    tok, named, wgu, wd, rows, slots, acc, part, ret, mixed,
    tok_sem, in_sem, w_sem, d_sem, id_s, id_r, ga_s, ga_r, di_s, di_r, re_s, re_r, sc_s, sc_r, go,
):
    g = lax.axis_index("group")
    z = lax.axis_index("expert")
    d = lax.axis_index("dp")
    lead = sets - 1
    own, width = tokens.shape
    cuts = pieces(width, FORWARD)
    back_cuts = pieces(width, BACK)
    cap = CAPG
    peer = [partner(g, m, groups) for m in range(groups)]
    far = [partner(z, m, experts) for m in range(experts)]
    group_order = list(range(groups - 1, -1, -1))
    expert_order = list(range(experts - 1, -1, -1))
    away = [ends_first(z, k, experts) for k in range(experts - 1)]
    barrier = pltpu.get_barrier_semaphore()

    tok_in = pltpu.make_async_copy(tokens, tok.at[d, g], tok_sem)
    tok_in.start()
    pltpu.make_async_copy(ids, named.at[d, 0], in_sem).start()
    pltpu.make_async_copy(codes, named.at[d, 1], in_sem).start()
    named_in = pltpu.make_async_copy(named.at[d], named.at[d], in_sem)

    def greet(**to):
        pl.semaphore_signal(barrier, inc=1, device_id=to, device_id_type=MESH)

    def remote(to, src, dst, send, recv):
        return pltpu.make_async_remote_copy(
            src_ref=src, dst_ref=dst, send_sem=send, recv_sem=recv,
            device_id=to, device_id_type=MESH,
        )

    def landed(ref, sem):
        pltpu.make_async_copy(ref, ref, sem).wait()

    def load():
        for c, cut in enumerate(cuts):
            pltpu.make_async_copy(w_gate.at[cut, :], wgu.at[0, cut, :], w_sem.at[c]).start()
            pltpu.make_async_copy(w_up.at[cut, :], wgu.at[1, cut, :], w_sem.at[c]).start()
        for c, cut in enumerate(back_cuts):
            pltpu.make_async_copy(w_down.at[:, cut], wd.at[:, cut], d_sem.at[c]).start()

    def send_tokens(order):
        for cut, sem in zip(cuts, range(len(cuts))):
            for m in order:
                remote(
                    {"group": peer[m], "dp": lead}, tok.at[d, g, :, cut], tok.at[d, g, :, cut],
                    ga_s, ga_r.at[sem, d],
                ).start()

    def give(c, cut, t):
        remote(
            {"expert": t, "dp": lead}, part.at[t, :, cut], ret.at[d, z, :, cut],
            re_s, re_r.at[c, d],
        ).start()

    def compute(present, urgent, later):
        for c, cut in enumerate(cuts):
            landed(slots.at[pl.ds(0, present), :, cut], di_r.at[c])
            landed(wgu.at[:, cut, :], w_sem.at[c])
            flat = slots[:, :, cut].reshape(experts * cap, cut.size)
            for i in range(2):
                made = dot(flat, wgu[i, cut, :])
                acc[i] = made if c == 0 else acc[i] + made
        hidden = (acc[0] / (1.0 + jnp.exp(-acc[0])) * acc[1]).astype(jnp.bfloat16)
        for c, cut in enumerate(back_cuts):
            landed(wd.at[:, cut], d_sem.at[c])
            made = dot(hidden, wd[:, cut]).astype(jnp.bfloat16)
            part[:, :, cut] = made.reshape(experts, cap, cut.size)
            for t in urgent:
                give(c, cut, t)
            if present < experts:
                ret[lead, z, :, cut] = part[z, :, cut]
        for c, cut in enumerate(back_cuts):
            for t in later:
                give(c, cut, t)

    @pl.when(d == lead)
    def _():
        for m in range(1, groups):
            greet(group=peer[m])
        for m in range(1, experts):
            for s in range(lead):
                greet(expert=far[m], dp=s)
        load()
        tok_in.wait()
        pl.semaphore_wait(barrier, groups - 1 + lead)
        for s in range(lead):
            pl.semaphore_signal(go, inc=1, device_id={"dp": s}, device_id_type=MESH)
        send_tokens(group_order[:-1])

        named_in.wait()
        routes = {lead: routing(named[lead, 0], named[lead, 1], experts, cap)}
        for s in range(lead):
            landed(named.at[s], id_r.at[s])
            routes[s] = routing(named[s, 0], named[s, 1], experts, cap)

        for s in range(lead, -1, -1):
            for c, cut in enumerate(cuts):
                landed(tok.at[s, pl.ds(0, groups - 1 if s == lead else groups), :, cut], ga_r.at[c, s])
                chosen = dot(routes[s][0], tok[s, :, :, cut].reshape(groups * own, cut.size))
                rows[s, :, :, cut] = chosen.astype(jnp.bfloat16).reshape(experts, cap, cut.size)
                if (s, c) == (lead, 0):
                    pl.semaphore_wait(go, lead)
                for m in expert_order:
                    if (s, m) != (lead, 0):
                        remote(
                            {"expert": far[m], "dp": s}, rows.at[s, far[m], :, cut], slots.at[z, :, cut],
                            di_s.at[s], di_r.at[c],
                        ).start()
                if s == lead:
                    slots[z, :, cut] = rows[s, z, :, cut]

        compute(experts - 1, away[:URGENT], away[URGENT:])

        for s in range(lead, -1, -1):
            for c, cut in enumerate(back_cuts):
                landed(ret.at[s, pl.ds(0, experts - 1 if s == lead else experts), :, cut], re_r.at[c, s])
                both = dot(routes[s][1], ret[s, :, :, cut].reshape(experts * cap, cut.size))
                total = (both[: groups * own] + both[groups * own :]).astype(jnp.bfloat16)
                mixed[s, :, :, cut] = total.reshape(groups, own, cut.size)
                for m in group_order:
                    if (s, m) != (lead, 0):
                        remote(
                            {"group": peer[m], "dp": s}, mixed.at[s, peer[m], :, cut], red.at[g, :, cut],
                            sc_s.at[s], sc_r.at[c],
                        ).start()
                if s == lead:
                    pltpu.make_async_copy(mixed.at[s, g, :, cut], red.at[g, :, cut], sc_r.at[c]).start()

        landed(tok.at[lead, pl.ds(0, groups - 1)], ga_s)
        landed(part.at[pl.ds(0, experts - 1)], re_s)
        for s in range(sets):
            landed(rows.at[s, pl.ds(0, experts - 1 if s == lead else experts)], di_s.at[s])
            landed(mixed.at[s, pl.ds(0, groups - 1 if s == lead else groups)], sc_s.at[s])

    @pl.when(d != lead)
    def _():
        greet(dp=lead)
        for m in range(1, experts):
            greet(expert=far[m])
        load()
        tok_in.wait()
        named_in.wait()
        pl.semaphore_wait(go, 1)
        send_tokens(group_order)
        remote({"dp": lead}, named.at[d], named.at[d], id_s, id_r.at[d]).start()
        pl.semaphore_wait(barrier, 2 * (experts - 1))
        pl.semaphore_signal(go, inc=1, device_id={"dp": lead}, device_id_type=MESH)

        compute(experts, away[:URGENT] + [z], away[URGENT:])

        landed(tok.at[d], ga_s)
        landed(named.at[d], id_s)
        landed(part, re_s)

    for c, cut in enumerate(back_cuts):
        landed(red.at[:, :, cut], sc_r.at[c])


def per_device(tokens, expert_ids, gate_codes, w_gate, w_up, w_down):
    groups = lax.axis_size("group")
    experts = lax.axis_size("expert")
    sets = lax.axis_size("dp")
    own, width = tokens.shape[1:]
    hid = w_gate.shape[2]
    bf16 = jnp.bfloat16
    any_space = pl.BlockSpec(memory_space=pl.ANY)
    dma = pltpu.SemaphoreType.DMA
    shares = pl.pallas_call(
        functools.partial(kernel, groups, experts, sets),
        out_shape=pltpu.VMEM((groups, own, width), bf16),
        in_specs=[any_space] * 6,
        out_specs=pl.BlockSpec(memory_space=pltpu.VMEM),
        scratch_shapes=[
            pltpu.VMEM((sets, groups, own, width), bf16),
            pltpu.VMEM((sets, 2, *expert_ids.shape[:0:-1]), jnp.int32),
            pltpu.VMEM((2, width, hid), bf16),
            pltpu.VMEM((hid, width), bf16),
            pltpu.VMEM((sets, experts, CAPG, width), bf16),
            pltpu.VMEM((experts, CAPG, width), bf16),
            pltpu.VMEM((2, experts * CAPG, hid), jnp.float32),
            pltpu.VMEM((experts, CAPG, width), bf16),
            pltpu.VMEM((sets, experts, CAPG, width), bf16),
            pltpu.VMEM((sets, groups, own, width), bf16),
            dma,
            dma,
            dma((len(FORWARD),)),
            dma((len(BACK),)),
            dma,
            dma((sets - 1,)),
            dma,
            dma((len(FORWARD), sets)),
            dma((sets,)),
            dma((len(FORWARD),)),
            dma,
            dma((len(BACK), sets)),
            dma((sets,)),
            dma((len(BACK),)),
            pltpu.SemaphoreType.REGULAR,
        ],
        compiler_params=pltpu.CompilerParams(
            collective_id=0, has_side_effects=True, vmem_limit_bytes=60 * 1024 * 1024
        ),
    )(tokens[0], expert_ids[0].T, gate_codes[0].T, w_gate[0], w_up[0], w_down[0])
    total = shares[0].astype(jnp.float32)
    for k in range(1, groups):
        total = total + shares[k].astype(jnp.float32)
    return total.astype(bf16)[None]


def solution(mesh):
    placed = (
        P(("expert", "dp"), "group", None),
        P(("expert", "dp"), None, None),
        P(("expert", "dp"), None, None),
        P("expert", None, "group"),
        P("expert", None, "group"),
        P("expert", "group", None),
    )
    return jax.shard_map(
        per_device,
        mesh=mesh,
        in_specs=placed,
        out_specs=P(("expert", "dp"), "group", None),
        check_vma=False,
    )
```

```python
import functools

import jax
import jax.numpy as jnp
from jax import lax
from jax.experimental import pallas as pl
from jax.experimental.pallas import tpu as pltpu
from jax.sharding import PartitionSpec as P

CAPG = 4
FORWARD = (2, 2, 2, 1)
BACK = (1, 2, 2, 2)
URGENT = 1
RELAY = 2
AFTER = 4
MESH = pl.DeviceIdType.MESH


def dot(a, b):
    return jnp.dot(a, b, preferred_element_type=jnp.float32)


def routing(ids, codes, experts, capacity):
    tokens = ids.shape[1]
    wide = experts * capacity
    codes = codes.astype(jnp.float32)
    gates = 2.5 * codes / jnp.sum(codes, axis=0, keepdims=True)
    slot = lax.broadcasted_iota(jnp.int32, (wide, tokens), 0)
    member = jnp.zeros((wide, tokens), jnp.float32)
    weight = jnp.zeros((wide, tokens), jnp.float32)
    for e in range(experts):
        hits = ids == e
        named = jnp.max(jnp.where(hits, 1.0, 0.0), axis=0, keepdims=True)
        gate = jnp.sum(jnp.where(hits, gates, 0.0), axis=0, keepdims=True)
        mine = (slot >= e * capacity) & (slot < (e + 1) * capacity)
        member = jnp.where(mine, named, member)
        weight = jnp.where(mine, gate, weight)
    row = lax.broadcasted_iota(jnp.int32, (tokens, tokens), 0)
    column = lax.broadcasted_iota(jnp.int32, (tokens, tokens), 1)
    before = jnp.where(row < column, 1.0, 0.0).astype(jnp.bfloat16)
    rank = dot(member.astype(jnp.bfloat16), before)
    place = jnp.where(rank == (slot % capacity).astype(jnp.float32), member, 0.0)
    mix = place * weight
    high = mix.astype(jnp.bfloat16)
    low = (mix - high.astype(jnp.float32)).astype(jnp.bfloat16)
    return place.astype(jnp.bfloat16), jnp.concatenate([flipped(high), flipped(low)], axis=0)


def flipped(a):
    n = a.shape[1]
    row = lax.broadcasted_iota(jnp.int32, (n, n), 0)
    column = lax.broadcasted_iota(jnp.int32, (n, n), 1)
    eye = jnp.where(row == column, 1.0, 0.0).astype(jnp.bfloat16)
    return lax.dot_general(
        eye, a, (((1,), (1,)), ((), ())), preferred_element_type=jnp.float32
    ).astype(jnp.bfloat16)


def pieces(width, shares):
    ends = [0]
    for k in range(len(shares)):
        ends.append(width * sum(shares[: k + 1]) // sum(shares) // 128 * 128)
    return [pl.ds(a, b - a) for a, b in zip(ends[:-1], ends[1:])]


def turns(sets, chunks, skip, after):
    last = sets - 1
    others = [(s, c) for s in range(last) for c in range(chunks)]
    return others[:after] + [(last, c) for c in range(skip, chunks)] + others[after:]


def relayed(width, groups):
    ends = [cut.start + cut.size for cut in pieces(width, FORWARD)][:RELAY]
    return ends[-1] if ends and ends[-1] % (128 * groups) == 0 else 0


def partner(a, m, n):
    out, bit = 0, 1
    while bit < n:
        out = out + bit * lax.rem(lax.div(a, bit) + m // bit % 2, 2)
        bit *= 2
    return out


def ends_first(z, k, n):
    at = jnp.where(z == 0, 0, jnp.where(z == n - 1, 1, z + 1))
    i = k + jnp.where(k >= at, 1, 0)
    return jnp.where(i == 0, 0, jnp.where(i == 1, n - 1, i - 1))


def kernel(
    groups, experts, sets, tokens, ids, codes, w_gate, w_up, w_down, red,
    tok, tok_sub, named, wgu, wd, rows, row_sub, hold, slots, acc, part, ret, mixed,
    tok_sem, in_sem, w_sem, d_sem, id_s, id_r, ga_s, ga_r, di_s, di_r, re_s, re_r, sc_s, sc_r, su_s, su_r, go,
):
    g = lax.axis_index("group")
    z = lax.axis_index("expert")
    d = lax.axis_index("dp")
    lead = sets - 1
    own, width = tokens.shape
    cuts = pieces(width, FORWARD)
    back_cuts = pieces(width, BACK)
    cap = CAPG
    skipped = relayed(width, groups)
    relay = skipped > 0
    skip = RELAY if relay else 0
    sub = skipped // groups
    peer = [partner(g, m, groups) for m in range(groups)]
    far = [partner(z, m, experts) for m in range(experts)]
    subs = [pl.ds(pl.multiple_of(p * sub, 128), sub) for p in peer] if relay else []
    group_order = list(range(groups - 1, -1, -1))
    expert_order = list(range(experts - 1, -1, -1))
    away = [ends_first(z, k, experts) for k in range(experts - 1)]
    barrier = pltpu.get_barrier_semaphore()

    tok_in = pltpu.make_async_copy(tokens, tok.at[d, g], tok_sem)
    tok_in.start()
    pltpu.make_async_copy(ids, named.at[d, 0], in_sem).start()
    pltpu.make_async_copy(codes, named.at[d, 1], in_sem).start()
    named_in = pltpu.make_async_copy(named.at[d], named.at[d], in_sem)

    def greet(**to):
        pl.semaphore_signal(barrier, inc=1, device_id=to, device_id_type=MESH)

    def remote(to, src, dst, send, recv):
        return pltpu.make_async_remote_copy(
            src_ref=src, dst_ref=dst, send_sem=send, recv_sem=recv,
            device_id=to, device_id_type=MESH,
        )

    def landed(ref, sem):
        pltpu.make_async_copy(ref, ref, sem).wait()

    def load():
        for c, cut in enumerate(cuts):
            pltpu.make_async_copy(w_gate.at[cut, :], wgu.at[0, cut, :], w_sem.at[c]).start()
            pltpu.make_async_copy(w_up.at[cut, :], wgu.at[1, cut, :], w_sem.at[c]).start()
        for cut in back_cuts:
            pltpu.make_async_copy(w_down.at[:, cut], wd.at[:, cut], d_sem).start()

    def send_tokens(which, order):
        for cut in which:
            sem = cuts.index(cut)
            for m in order:
                remote(
                    {"group": peer[m], "dp": lead}, tok.at[d, g, :, cut], tok.at[d, g, :, cut],
                    ga_s, ga_r.at[sem, d],
                ).start()

    def give(c, cut, t):
        remote(
            {"expert": t, "dp": lead}, part.at[t, :, cut], ret.at[lead - d, z, :, cut],
            re_s, re_r.at[c, lead - d],
        ).start()

    def compute(present, urgent, later):
        line = list(range(len(cuts)))
        if present == experts:
            line = line[skip:] + line[:skip]
        for c in line:
            cut = cuts[c]
            if present < experts or c >= skip:
                landed(slots.at[pl.ds(0, present), :, cut], di_r.at[c])
            elif c == 0:
                landed(slots.at[:, :, pl.ds(0, skipped)], su_r.at[2])
            landed(wgu.at[:, cut, :], w_sem.at[c])
            flat = slots[:, :, cut].reshape(experts * cap, cut.size)
            for i in range(2):
                made = dot(flat, wgu[i, cut, :])
                acc[i] = made if c == line[0] else acc[i] + made
        hidden = (acc[0] / (1.0 + jnp.exp(-acc[0])) * acc[1]).astype(jnp.bfloat16)
        landed(wd, d_sem)
        for c, cut in enumerate(back_cuts):
            made = dot(hidden, wd[:, cut]).astype(jnp.bfloat16)
            part[:, :, cut] = made.reshape(experts, cap, cut.size)
            for t in urgent:
                give(c, cut, t)
            if present < experts:
                ret[0, z, :, cut] = part[z, :, cut]
        for c, cut in enumerate(back_cuts):
            for t in later:
                give(c, cut, t)

    @pl.when(d == lead)
    def _():
        for m in range(1, groups):
            greet(group=peer[m])
        for m in range(1, experts):
            for s in range(lead):
                greet(expert=far[m], dp=s)
        load()
        tok_in.wait()
        pl.semaphore_wait(barrier, groups - 1 + lead)
        for s in range(lead):
            pl.semaphore_signal(go, inc=1, device_id={"dp": s}, device_id_type=MESH)
        if relay:
            for m in group_order[:-1]:
                remote(
                    {"group": peer[m]}, tok.at[lead, g, :, subs[m]], tok_sub.at[g], ga_s, su_r.at[0]
                ).start()
            tok_sub[g] = tok[lead, g, :, subs[0]]
        send_tokens(cuts[skip:], group_order[:-1])

        named_in.wait()
        routes = {lead: routing(named[lead, 0], named[lead, 1], experts, cap)}
        for s in range(lead):
            landed(named.at[s], id_r.at[s])
            routes[s] = routing(named[s, 0], named[s, 1], experts, cap)

        if relay:
            landed(tok_sub.at[pl.ds(0, groups - 1)], su_r.at[0])
            chosen = dot(routes[lead][0], tok_sub[...].reshape(groups * own, sub))
            row_sub[...] = chosen.astype(jnp.bfloat16).reshape(experts, cap, sub)
        pl.semaphore_wait(go, lead)
        if relay:
            for m in expert_order[:-1]:
                remote({"expert": far[m]}, row_sub.at[far[m]], hold.at[z], su_s.at[0], su_r.at[1]).start()
            hold[z] = row_sub[z]

        for s, c in turns(sets, len(cuts), skip, AFTER):
            cut = cuts[c]
            landed(tok.at[s, pl.ds(0, groups - 1 if s == lead else groups), :, cut], ga_r.at[c, s])
            chosen = dot(routes[s][0], tok[s, :, :, cut].reshape(groups * own, cut.size))
            rows[s, :, :, cut] = chosen.astype(jnp.bfloat16).reshape(experts, cap, cut.size)
            for m in expert_order:
                if (s, m) != (0, 0):
                    remote(
                        {"expert": far[m], "dp": lead - s}, rows.at[s, far[m], :, cut], slots.at[z, :, cut],
                        di_s.at[s], di_r.at[c],
                    ).start()
            if s == 0:
                slots[z, :, cut] = rows[s, z, :, cut]

        if relay:
            landed(hold.at[pl.ds(0, experts - 1)], su_r.at[1])
            for m in group_order:
                remote(
                    {"group": peer[m], "dp": 0}, hold, slots.at[:, :, subs[0]], su_s.at[1], su_r.at[2]
                ).start()

        compute(experts - 1, away[:URGENT], away[URGENT:])

        for s, c in turns(sets, len(back_cuts), 0, len(back_cuts) * lead):
            cut = back_cuts[c]
            landed(ret.at[s, pl.ds(0, experts if s else experts - 1), :, cut], re_r.at[c, s])
            both = dot(routes[s][1], ret[s, :, :, cut].reshape(experts * cap, cut.size))
            total = (both[: groups * own] + both[groups * own :]).astype(jnp.bfloat16)
            mixed[s, :, :, cut] = total.reshape(groups, own, cut.size)
            for m in group_order:
                if (s, m) != (lead, 0):
                    remote(
                        {"group": peer[m], "dp": s}, mixed.at[s, peer[m], :, cut], red.at[g, :, cut],
                        sc_s.at[s], sc_r.at[c],
                    ).start()
            if s == lead:
                pltpu.make_async_copy(mixed.at[s, g, :, cut], red.at[g, :, cut], sc_r.at[c]).start()

        if relay:
            landed(row_sub.at[pl.ds(0, experts - 1)], su_s.at[0])
            landed(rows.at[lead, :, :, pl.ds(0, skipped)], su_s.at[1])
        landed(tok.at[lead, pl.ds(0, groups - 1), :, pl.ds(0, width - skipped + sub)], ga_s)
        landed(part.at[pl.ds(0, experts - 1)], re_s)
        for s in range(sets):
            kept = width - skipped if s == lead else width
            landed(rows.at[s, pl.ds(0, experts if s else experts - 1), :, pl.ds(0, kept)], di_s.at[s])
            landed(mixed.at[s, pl.ds(0, groups - 1 if s == lead else groups)], sc_s.at[s])

    @pl.when(d != lead)
    def _():
        greet(dp=lead)
        for m in range(1, experts):
            greet(expert=far[m])
        load()
        tok_in.wait()
        named_in.wait()
        pl.semaphore_wait(go, 1)
        send_tokens(cuts, group_order)
        remote({"dp": lead}, named.at[d], named.at[d], id_s, id_r.at[d]).start()
        pl.semaphore_wait(barrier, 2 * (experts - 1))
        pl.semaphore_signal(go, inc=1, device_id={"dp": lead}, device_id_type=MESH)

        compute(experts, away[:URGENT] + [z], away[URGENT:])

        landed(tok.at[d], ga_s)
        landed(named.at[d], id_s)
        landed(part, re_s)

    for c, cut in enumerate(back_cuts):
        landed(red.at[:, :, cut], sc_r.at[c])


def per_device(tokens, expert_ids, gate_codes, w_gate, w_up, w_down):
    groups = lax.axis_size("group")
    experts = lax.axis_size("expert")
    sets = lax.axis_size("dp")
    own, width = tokens.shape[1:]
    hid = w_gate.shape[2]
    bf16 = jnp.bfloat16
    sub = max(128, relayed(width, groups) // groups)
    any_space = pl.BlockSpec(memory_space=pl.ANY)
    dma = pltpu.SemaphoreType.DMA
    shares = pl.pallas_call(
        functools.partial(kernel, groups, experts, sets),
        out_shape=pltpu.VMEM((groups, own, width), bf16),
        in_specs=[any_space] * 6,
        out_specs=pl.BlockSpec(memory_space=pltpu.VMEM),
        scratch_shapes=[
            pltpu.VMEM((sets, groups, own, width), bf16),
            pltpu.VMEM((groups, own, sub), bf16),
            pltpu.VMEM((sets, 2, *expert_ids.shape[:0:-1]), jnp.int32),
            pltpu.VMEM((2, width, hid), bf16),
            pltpu.VMEM((hid, width), bf16),
            pltpu.VMEM((sets, experts, CAPG, width), bf16),
            pltpu.VMEM((experts, CAPG, sub), bf16),
            pltpu.VMEM((experts, CAPG, sub), bf16),
            pltpu.VMEM((experts, CAPG, width), bf16),
            pltpu.VMEM((2, experts * CAPG, hid), jnp.float32),
            pltpu.VMEM((experts, CAPG, width), bf16),
            pltpu.VMEM((sets, experts, CAPG, width), bf16),
            pltpu.VMEM((sets, groups, own, width), bf16),
            dma,
            dma,
            dma((len(FORWARD),)),
            dma,
            dma,
            dma((sets - 1,)),
            dma,
            dma((len(FORWARD), sets)),
            dma((sets,)),
            dma((len(FORWARD),)),
            dma,
            dma((len(BACK), sets)),
            dma((sets,)),
            dma((len(BACK),)),
            dma((2,)),
            dma((3,)),
            pltpu.SemaphoreType.REGULAR,
        ],
        compiler_params=pltpu.CompilerParams(
            collective_id=0, has_side_effects=True, vmem_limit_bytes=60 * 1024 * 1024
        ),
    )(tokens[0], expert_ids[0].T, gate_codes[0].T, w_gate[0], w_up[0], w_down[0])
    total = shares[0].astype(jnp.float32)
    for k in range(1, groups):
        total = total + shares[k].astype(jnp.float32)
    return total.astype(bf16)[None]


def solution(mesh):
    placed = (
        P(("expert", "dp"), "group", None),
        P(("expert", "dp"), None, None),
        P(("expert", "dp"), None, None),
        P("expert", None, "group"),
        P("expert", None, "group"),
        P("expert", "group", None),
    )
    return jax.shard_map(
        per_device,
        mesh=mesh,
        in_specs=placed,
        out_specs=P(("expert", "dp"), "group", None),
        check_vma=False,
    )
```

```python
import functools

import jax
import jax.numpy as jnp
from jax import lax
from jax.experimental import pallas as pl
from jax.experimental.pallas import tpu as pltpu
from jax.sharding import PartitionSpec as P

CAPG = 4
FORWARD = (2, 2, 2, 1)
BACK = (1, 1, 1, 1)
URGENT = 1
RELAY = 2
AFTER = 4
MESH = pl.DeviceIdType.MESH


def dot(a, b):
    return jnp.dot(a, b, preferred_element_type=jnp.float32)


def routing(ids, codes, experts, capacity):
    tokens = ids.shape[1]
    wide = experts * capacity
    codes = codes.astype(jnp.float32)
    gates = 2.5 * codes / jnp.sum(codes, axis=0, keepdims=True)
    slot = lax.broadcasted_iota(jnp.int32, (wide, tokens), 0)
    member = jnp.zeros((wide, tokens), jnp.float32)
    weight = jnp.zeros((wide, tokens), jnp.float32)
    for e in range(experts):
        hits = ids == e
        named = jnp.max(jnp.where(hits, 1.0, 0.0), axis=0, keepdims=True)
        gate = jnp.sum(jnp.where(hits, gates, 0.0), axis=0, keepdims=True)
        mine = (slot >= e * capacity) & (slot < (e + 1) * capacity)
        member = jnp.where(mine, named, member)
        weight = jnp.where(mine, gate, weight)
    row = lax.broadcasted_iota(jnp.int32, (tokens, tokens), 0)
    column = lax.broadcasted_iota(jnp.int32, (tokens, tokens), 1)
    before = jnp.where(row < column, 1.0, 0.0).astype(jnp.bfloat16)
    rank = dot(member.astype(jnp.bfloat16), before)
    place = jnp.where(rank == (slot % capacity).astype(jnp.float32), member, 0.0)
    mix = place * weight
    high = mix.astype(jnp.bfloat16)
    low = (mix - high.astype(jnp.float32)).astype(jnp.bfloat16)
    return place.astype(jnp.bfloat16), jnp.concatenate([flipped(high), flipped(low)], axis=0)


def flipped(a):
    n = a.shape[1]
    row = lax.broadcasted_iota(jnp.int32, (n, n), 0)
    column = lax.broadcasted_iota(jnp.int32, (n, n), 1)
    eye = jnp.where(row == column, 1.0, 0.0).astype(jnp.bfloat16)
    return lax.dot_general(
        eye, a, (((1,), (1,)), ((), ())), preferred_element_type=jnp.float32
    ).astype(jnp.bfloat16)


def pieces(width, shares):
    ends = [0]
    for k in range(len(shares)):
        ends.append(width * sum(shares[: k + 1]) // sum(shares) // 128 * 128)
    return [pl.ds(a, b - a) for a, b in zip(ends[:-1], ends[1:])]


def turns(sets, chunks, skip, after):
    last = sets - 1
    others = [(s, c) for s in range(last) for c in range(chunks)]
    return others[:after] + [(last, c) for c in range(skip, chunks)] + others[after:]


def relayed(width, groups):
    ends = [cut.start + cut.size for cut in pieces(width, FORWARD)][:RELAY]
    return ends[-1] if ends and ends[-1] % (128 * groups) == 0 else 0


def partner(a, m, n):
    out, bit = 0, 1
    while bit < n:
        out = out + bit * lax.rem(lax.div(a, bit) + m // bit % 2, 2)
        bit *= 2
    return out


def ends_first(z, k, n):
    at = jnp.where(z == 0, 0, jnp.where(z == n - 1, 1, z + 1))
    i = k + jnp.where(k >= at, 1, 0)
    return jnp.where(i == 0, 0, jnp.where(i == 1, n - 1, i - 1))


def kernel(
    groups, experts, sets, tokens, ids, codes, w_gate, w_up, w_down, red,
    tok, tok_sub, named, wgu, wd, rows, row_sub, hold, slots, acc, part, ret, mixed,
    tok_sem, in_sem, w_sem, d_sem, id_s, id_r, ga_s, ga_r, di_s, di_r, re_s, re_r, sc_s, sc_r, su_s, su_r, go,
):
    g = lax.axis_index("group")
    z = lax.axis_index("expert")
    d = lax.axis_index("dp")
    lead = sets - 1
    own, width = tokens.shape
    cuts = pieces(width, FORWARD)
    back_cuts = pieces(width, BACK)
    cap = CAPG
    skipped = relayed(width, groups)
    relay = skipped > 0
    skip = RELAY if relay else 0
    sub = skipped // groups
    peer = [partner(g, m, groups) for m in range(groups)]
    far = [partner(z, m, experts) for m in range(experts)]
    subs = [pl.ds(pl.multiple_of(p * sub, 128), sub) for p in peer] if relay else []
    group_order = list(range(groups - 1, -1, -1))
    expert_order = list(range(experts - 1, -1, -1))
    away = [ends_first(z, k, experts) for k in range(experts - 1)]
    barrier = pltpu.get_barrier_semaphore()

    tok_in = pltpu.make_async_copy(tokens, tok.at[d, g], tok_sem)
    tok_in.start()
    pltpu.make_async_copy(ids, named.at[d, 0], in_sem).start()
    pltpu.make_async_copy(codes, named.at[d, 1], in_sem).start()
    named_in = pltpu.make_async_copy(named.at[d], named.at[d], in_sem)

    def greet(**to):
        pl.semaphore_signal(barrier, inc=1, device_id=to, device_id_type=MESH)

    def remote(to, src, dst, send, recv):
        return pltpu.make_async_remote_copy(
            src_ref=src, dst_ref=dst, send_sem=send, recv_sem=recv,
            device_id=to, device_id_type=MESH,
        )

    def landed(ref, sem):
        pltpu.make_async_copy(ref, ref, sem).wait()

    def load():
        for c, cut in enumerate(cuts):
            pltpu.make_async_copy(w_gate.at[cut, :], wgu.at[0, cut, :], w_sem.at[c]).start()
            pltpu.make_async_copy(w_up.at[cut, :], wgu.at[1, cut, :], w_sem.at[c]).start()
        for cut in back_cuts:
            pltpu.make_async_copy(w_down.at[:, cut], wd.at[:, cut], d_sem).start()

    def send_tokens(which, order):
        for cut in which:
            sem = cuts.index(cut)
            for m in order:
                remote(
                    {"group": peer[m], "dp": lead}, tok.at[d, g, :, cut], tok.at[d, g, :, cut],
                    ga_s, ga_r.at[sem, d],
                ).start()

    def give(c, cut, t):
        remote(
            {"expert": t, "dp": lead}, part.at[t, :, cut], ret.at[lead - d, z, :, cut],
            re_s, re_r.at[c, lead - d],
        ).start()

    def compute(present, urgent, later):
        line = list(range(len(cuts)))
        if present == experts:
            line = line[skip:] + line[:skip]
        for c in line:
            cut = cuts[c]
            if present < experts or c >= skip:
                landed(slots.at[pl.ds(0, present), :, cut], di_r.at[c])
            elif c == 0:
                landed(slots.at[:, :, pl.ds(0, skipped)], su_r.at[2])
            landed(wgu.at[:, cut, :], w_sem.at[c])
            flat = slots[:, :, cut].reshape(experts * cap, cut.size)
            for i in range(2):
                made = dot(flat, wgu[i, cut, :])
                acc[i] = made if c == line[0] else acc[i] + made
        hidden = (acc[0] / (1.0 + jnp.exp(-acc[0])) * acc[1]).astype(jnp.bfloat16)
        landed(wd, d_sem)
        made = dot(hidden, wd[:, back_cuts[0]])
        for c, cut in enumerate(back_cuts):
            ready = made.astype(jnp.bfloat16)
            if c + 1 < len(back_cuts):
                made = dot(hidden, wd[:, back_cuts[c + 1]])
            part[:, :, cut] = ready.reshape(experts, cap, cut.size)
            for t in urgent:
                give(c, cut, t)
            if present < experts:
                ret[0, z, :, cut] = part[z, :, cut]
        for c, cut in enumerate(back_cuts):
            for t in later:
                give(c, cut, t)

    @pl.when(d == lead)
    def _():
        for m in range(1, groups):
            greet(group=peer[m])
        for m in range(1, experts):
            for s in range(lead):
                greet(expert=far[m], dp=s)
        load()
        tok_in.wait()
        pl.semaphore_wait(barrier, groups - 1 + lead)
        for s in range(lead):
            pl.semaphore_signal(go, inc=1, device_id={"dp": s}, device_id_type=MESH)
        if relay:
            for m in group_order[:-1]:
                remote(
                    {"group": peer[m]}, tok.at[lead, g, :, subs[m]], tok_sub.at[g], ga_s, su_r.at[0]
                ).start()
            tok_sub[g] = tok[lead, g, :, subs[0]]
        send_tokens(cuts[skip:], group_order[:-1])

        named_in.wait()
        routes = {lead: routing(named[lead, 0], named[lead, 1], experts, cap)}
        for s in range(lead):
            landed(named.at[s], id_r.at[s])
            routes[s] = routing(named[s, 0], named[s, 1], experts, cap)

        if relay:
            landed(tok_sub.at[pl.ds(0, groups - 1)], su_r.at[0])
            chosen = dot(routes[lead][0], tok_sub[...].reshape(groups * own, sub))
            row_sub[...] = chosen.astype(jnp.bfloat16).reshape(experts, cap, sub)
        pl.semaphore_wait(go, lead)
        if relay:
            for m in expert_order[:-1]:
                remote({"expert": far[m]}, row_sub.at[far[m]], hold.at[z], su_s.at[0], su_r.at[1]).start()
            hold[z] = row_sub[z]

        for s, c in turns(sets, len(cuts), skip, AFTER):
            cut = cuts[c]
            landed(tok.at[s, pl.ds(0, groups - 1 if s == lead else groups), :, cut], ga_r.at[c, s])
            chosen = dot(routes[s][0], tok[s, :, :, cut].reshape(groups * own, cut.size))
            rows[s, :, :, cut] = chosen.astype(jnp.bfloat16).reshape(experts, cap, cut.size)
            for m in expert_order:
                if (s, m) != (0, 0):
                    remote(
                        {"expert": far[m], "dp": lead - s}, rows.at[s, far[m], :, cut], slots.at[z, :, cut],
                        di_s.at[s], di_r.at[c],
                    ).start()
            if s == 0:
                slots[z, :, cut] = rows[s, z, :, cut]

        if relay:
            landed(hold.at[pl.ds(0, experts - 1)], su_r.at[1])
            for m in group_order:
                remote(
                    {"group": peer[m], "dp": 0}, hold, slots.at[:, :, subs[0]], su_s.at[1], su_r.at[2]
                ).start()

        compute(experts - 1, away, [])

        for s, c in turns(sets, len(back_cuts), 0, len(back_cuts) * lead):
            cut = back_cuts[c]
            landed(ret.at[s, pl.ds(0, experts if s else experts - 1), :, cut], re_r.at[c, s])
            both = dot(routes[s][1], ret[s, :, :, cut].reshape(experts * cap, cut.size))
            total = (both[: groups * own] + both[groups * own :]).astype(jnp.bfloat16)
            mixed[s, :, :, cut] = total.reshape(groups, own, cut.size)
            for m in group_order:
                if (s, m) != (lead, 0):
                    remote(
                        {"group": peer[m], "dp": s}, mixed.at[s, peer[m], :, cut], red.at[g, :, cut],
                        sc_s.at[s], sc_r.at[c],
                    ).start()
            if s == lead:
                pltpu.make_async_copy(mixed.at[s, g, :, cut], red.at[g, :, cut], sc_r.at[c]).start()

        if relay:
            landed(row_sub.at[pl.ds(0, experts - 1)], su_s.at[0])
            landed(rows.at[lead, :, :, pl.ds(0, skipped)], su_s.at[1])
        landed(tok.at[lead, pl.ds(0, groups - 1), :, pl.ds(0, width - skipped + sub)], ga_s)
        landed(part.at[pl.ds(0, experts - 1)], re_s)
        for s in range(sets):
            kept = width - skipped if s == lead else width
            landed(rows.at[s, pl.ds(0, experts if s else experts - 1), :, pl.ds(0, kept)], di_s.at[s])
            landed(mixed.at[s, pl.ds(0, groups - 1 if s == lead else groups)], sc_s.at[s])

    @pl.when(d != lead)
    def _():
        greet(dp=lead)
        for m in range(1, experts):
            greet(expert=far[m])
        load()
        tok_in.wait()
        named_in.wait()
        pl.semaphore_wait(go, 1)
        send_tokens(cuts, group_order)
        remote({"dp": lead}, named.at[d], named.at[d], id_s, id_r.at[d]).start()
        pl.semaphore_wait(barrier, 2 * (experts - 1))
        pl.semaphore_signal(go, inc=1, device_id={"dp": lead}, device_id_type=MESH)

        compute(experts, away[:URGENT] + [z], away[URGENT:])

        landed(tok.at[d], ga_s)
        landed(named.at[d], id_s)
        landed(part, re_s)

    for c, cut in enumerate(back_cuts):
        landed(red.at[:, :, cut], sc_r.at[c])


def per_device(tokens, expert_ids, gate_codes, w_gate, w_up, w_down):
    groups = lax.axis_size("group")
    experts = lax.axis_size("expert")
    sets = lax.axis_size("dp")
    own, width = tokens.shape[1:]
    hid = w_gate.shape[2]
    bf16 = jnp.bfloat16
    sub = max(128, relayed(width, groups) // groups)
    any_space = pl.BlockSpec(memory_space=pl.ANY)
    dma = pltpu.SemaphoreType.DMA
    shares = pl.pallas_call(
        functools.partial(kernel, groups, experts, sets),
        out_shape=pltpu.VMEM((groups, own, width), bf16),
        in_specs=[any_space] * 6,
        out_specs=pl.BlockSpec(memory_space=pltpu.VMEM),
        scratch_shapes=[
            pltpu.VMEM((sets, groups, own, width), bf16),
            pltpu.VMEM((groups, own, sub), bf16),
            pltpu.VMEM((sets, 2, *expert_ids.shape[:0:-1]), jnp.int32),
            pltpu.VMEM((2, width, hid), bf16),
            pltpu.VMEM((hid, width), bf16),
            pltpu.VMEM((sets, experts, CAPG, width), bf16),
            pltpu.VMEM((experts, CAPG, sub), bf16),
            pltpu.VMEM((experts, CAPG, sub), bf16),
            pltpu.VMEM((experts, CAPG, width), bf16),
            pltpu.VMEM((2, experts * CAPG, hid), jnp.float32),
            pltpu.VMEM((experts, CAPG, width), bf16),
            pltpu.VMEM((sets, experts, CAPG, width), bf16),
            pltpu.VMEM((sets, groups, own, width), bf16),
            dma,
            dma,
            dma((len(FORWARD),)),
            dma,
            dma,
            dma((sets - 1,)),
            dma,
            dma((len(FORWARD), sets)),
            dma((sets,)),
            dma((len(FORWARD),)),
            dma,
            dma((len(BACK), sets)),
            dma((sets,)),
            dma((len(BACK),)),
            dma((2,)),
            dma((3,)),
            pltpu.SemaphoreType.REGULAR,
        ],
        compiler_params=pltpu.CompilerParams(
            collective_id=0, has_side_effects=True, vmem_limit_bytes=60 * 1024 * 1024
        ),
    )(tokens[0], expert_ids[0].T, gate_codes[0].T, w_gate[0], w_up[0], w_down[0])
    total = shares[0].astype(jnp.float32)
    for k in range(1, groups):
        total = total + shares[k].astype(jnp.float32)
    return total.astype(bf16)[None]


def solution(mesh):
    placed = (
        P(("expert", "dp"), "group", None),
        P(("expert", "dp"), None, None),
        P(("expert", "dp"), None, None),
        P("expert", None, "group"),
        P("expert", None, "group"),
        P("expert", "group", None),
    )
    return jax.shard_map(
        per_device,
        mesh=mesh,
        in_specs=placed,
        out_specs=P(("expert", "dp"), "group", None),
        check_vma=False,
    )
```

```python
import functools

import jax
import jax.numpy as jnp
from jax import lax
from jax.experimental import pallas as pl
from jax.experimental.pallas import tpu as pltpu
from jax.sharding import PartitionSpec as P

CAPG = 4
FORWARD = (2, 2, 2, 1)
BACK = (1, 1, 1, 1)
URGENT = 1
RELAY = 2
AFTER = 4
MESH = pl.DeviceIdType.MESH


def dot(a, b):
    return jnp.dot(a, b, preferred_element_type=jnp.float32)


def routing(ids, codes, experts, capacity):
    tokens = ids.shape[1]
    wide = experts * capacity
    codes = codes.astype(jnp.float32)
    gates = 2.5 * codes / jnp.sum(codes, axis=0, keepdims=True)
    slot = lax.broadcasted_iota(jnp.int32, (wide, tokens), 0)
    member = jnp.zeros((wide, tokens), jnp.float32)
    weight = jnp.zeros((wide, tokens), jnp.float32)
    for e in range(experts):
        hits = ids == e
        named = jnp.max(jnp.where(hits, 1.0, 0.0), axis=0, keepdims=True)
        gate = jnp.sum(jnp.where(hits, gates, 0.0), axis=0, keepdims=True)
        mine = (slot >= e * capacity) & (slot < (e + 1) * capacity)
        member = jnp.where(mine, named, member)
        weight = jnp.where(mine, gate, weight)
    row = lax.broadcasted_iota(jnp.int32, (tokens, tokens), 0)
    column = lax.broadcasted_iota(jnp.int32, (tokens, tokens), 1)
    before = jnp.where(row < column, 1.0, 0.0).astype(jnp.bfloat16)
    rank = dot(member.astype(jnp.bfloat16), before)
    place = jnp.where(rank == (slot % capacity).astype(jnp.float32), member, 0.0)
    mix = place * weight
    high = mix.astype(jnp.bfloat16)
    low = (mix - high.astype(jnp.float32)).astype(jnp.bfloat16)
    return place.astype(jnp.bfloat16), jnp.concatenate([flipped(high), flipped(low)], axis=0)


def flipped(a):
    n = a.shape[1]
    row = lax.broadcasted_iota(jnp.int32, (n, n), 0)
    column = lax.broadcasted_iota(jnp.int32, (n, n), 1)
    eye = jnp.where(row == column, 1.0, 0.0).astype(jnp.bfloat16)
    return lax.dot_general(
        eye, a, (((1,), (1,)), ((), ())), preferred_element_type=jnp.float32
    ).astype(jnp.bfloat16)


def pieces(width, shares):
    ends = [0]
    for k in range(len(shares)):
        ends.append(width * sum(shares[: k + 1]) // sum(shares) // 128 * 128)
    return [pl.ds(a, b - a) for a, b in zip(ends[:-1], ends[1:])]


def turns(sets, chunks, skip, after):
    last = sets - 1
    others = [(s, c) for s in range(last) for c in range(chunks)]
    return others[:after] + [(last, c) for c in range(skip, chunks)] + others[after:]


def relayed(width, groups):
    ends = [cut.start + cut.size for cut in pieces(width, FORWARD)][:RELAY]
    return ends[-1] if ends and ends[-1] % (128 * groups) == 0 else 0


def partner(a, m, n):
    out, bit = 0, 1
    while bit < n:
        out = out + bit * lax.rem(lax.div(a, bit) + m // bit % 2, 2)
        bit *= 2
    return out


def ends_first(z, k, n):
    at = jnp.where(z == 0, 0, jnp.where(z == n - 1, 1, z + 1))
    i = k + jnp.where(k >= at, 1, 0)
    return jnp.where(i == 0, 0, jnp.where(i == 1, n - 1, i - 1))


def kernel(
    groups, experts, sets, tokens, ids, codes, w_gate, w_up, w_down, out,
    red, tok, tok_sub, named, wgu, wd, rows, row_sub, hold, slots, acc, part, ret, mixed,
    tok_sem, in_sem, w_sem, d_sem, id_s, id_r, ga_s, ga_r, di_s, di_r, re_s, re_r, sc_s, sc_r, su_s, su_r, go,
):
    g = lax.axis_index("group")
    z = lax.axis_index("expert")
    d = lax.axis_index("dp")
    lead = sets - 1
    own, width = tokens.shape
    cuts = pieces(width, FORWARD)
    back_cuts = pieces(width, BACK)
    cap = CAPG
    skipped = relayed(width, groups)
    relay = skipped > 0
    skip = RELAY if relay else 0
    sub = skipped // groups
    peer = [partner(g, m, groups) for m in range(groups)]
    far = [partner(z, m, experts) for m in range(experts)]
    subs = [pl.ds(pl.multiple_of(p * sub, 128), sub) for p in peer] if relay else []
    group_order = list(range(groups - 1, -1, -1))
    expert_order = list(range(experts - 1, -1, -1))
    away = [ends_first(z, k, experts) for k in range(experts - 1)]
    barrier = pltpu.get_barrier_semaphore()

    tok_in = pltpu.make_async_copy(tokens, tok.at[d, g], tok_sem)
    tok_in.start()
    pltpu.make_async_copy(ids, named.at[d, 0], in_sem).start()
    pltpu.make_async_copy(codes, named.at[d, 1], in_sem).start()
    named_in = pltpu.make_async_copy(named.at[d], named.at[d], in_sem)

    def greet(**to):
        pl.semaphore_signal(barrier, inc=1, device_id=to, device_id_type=MESH)

    def remote(to, src, dst, send, recv):
        return pltpu.make_async_remote_copy(
            src_ref=src, dst_ref=dst, send_sem=send, recv_sem=recv,
            device_id=to, device_id_type=MESH,
        )

    def landed(ref, sem):
        pltpu.make_async_copy(ref, ref, sem).wait()

    def load():
        for cut in cuts:
            pltpu.make_async_copy(w_gate.at[cut, :], wgu.at[0, cut, :], w_sem).start()
            pltpu.make_async_copy(w_up.at[cut, :], wgu.at[1, cut, :], w_sem).start()
        for cut in back_cuts:
            pltpu.make_async_copy(w_down.at[:, cut], wd.at[:, cut], d_sem).start()

    def send_tokens(which, order):
        for cut in which:
            sem = cuts.index(cut)
            for m in order:
                remote(
                    {"group": peer[m], "dp": lead}, tok.at[d, g, :, cut], tok.at[d, g, :, cut],
                    ga_s, ga_r.at[sem, d],
                ).start()

    def give(c, cut, t):
        remote(
            {"expert": t, "dp": lead}, part.at[t, :, cut], ret.at[lead - d, z, :, cut],
            re_s, re_r.at[c, lead - d],
        ).start()

    def compute(present, urgent, later):
        line = list(range(len(cuts)))
        if present == experts:
            line = line[skip:] + line[:skip]
        for c in line:
            cut = cuts[c]
            if present < experts or c >= skip:
                landed(slots.at[pl.ds(0, present), :, cut], di_r.at[c])
            elif c == 0:
                landed(slots.at[:, :, pl.ds(0, skipped)], su_r.at[2])
            if c == line[0]:
                landed(wgu, w_sem)
            flat = slots[:, :, cut].reshape(experts * cap, cut.size)
            for i in range(2):
                made = dot(flat, wgu[i, cut, :])
                acc[i] = made if c == line[0] else acc[i] + made
        hidden = (acc[0] / (1.0 + jnp.exp(-acc[0])) * acc[1]).astype(jnp.bfloat16)
        landed(wd, d_sem)
        made = dot(hidden, wd[:, back_cuts[0]])
        for c, cut in enumerate(back_cuts):
            ready = made.astype(jnp.bfloat16)
            if c + 1 < len(back_cuts):
                made = dot(hidden, wd[:, back_cuts[c + 1]])
            part[:, :, cut] = ready.reshape(experts, cap, cut.size)
            for t in urgent:
                give(c, cut, t)
            if present < experts:
                ret[0, z, :, cut] = part[z, :, cut]
        for c, cut in enumerate(back_cuts):
            for t in later:
                give(c, cut, t)

    @pl.when(d == lead)
    def _():
        for m in range(1, groups):
            greet(group=peer[m])
        for m in range(1, experts):
            for s in range(lead):
                greet(expert=far[m], dp=s)
        load()
        tok_in.wait()
        pl.semaphore_wait(barrier, groups - 1 + lead)
        for s in range(lead):
            pl.semaphore_signal(go, inc=1, device_id={"dp": s}, device_id_type=MESH)
        if relay:
            for m in group_order[:-1]:
                remote(
                    {"group": peer[m]}, tok.at[lead, g, :, subs[m]], tok_sub.at[g], ga_s, su_r.at[0]
                ).start()
            tok_sub[g] = tok[lead, g, :, subs[0]]
        send_tokens(cuts[skip:], group_order[:-1])

        named_in.wait()
        routes = {lead: routing(named[lead, 0], named[lead, 1], experts, cap)}
        for s in range(lead):
            landed(named.at[s], id_r.at[s])
            routes[s] = routing(named[s, 0], named[s, 1], experts, cap)

        if relay:
            landed(tok_sub.at[pl.ds(0, groups - 1)], su_r.at[0])
            chosen = dot(routes[lead][0], tok_sub[...].reshape(groups * own, sub))
            row_sub[...] = chosen.astype(jnp.bfloat16).reshape(experts, cap, sub)
        pl.semaphore_wait(go, lead)
        if relay:
            for m in expert_order[:-1]:
                remote({"expert": far[m]}, row_sub.at[far[m]], hold.at[z], su_s.at[0], su_r.at[1]).start()
            hold[z] = row_sub[z]

        for s, c in turns(sets, len(cuts), skip, AFTER):
            cut = cuts[c]
            landed(tok.at[s, pl.ds(0, groups - 1 if s == lead else groups), :, cut], ga_r.at[c, s])
            chosen = dot(routes[s][0], tok[s, :, :, cut].reshape(groups * own, cut.size))
            rows[s, :, :, cut] = chosen.astype(jnp.bfloat16).reshape(experts, cap, cut.size)
            for m in expert_order:
                if (s, m) != (0, 0):
                    remote(
                        {"expert": far[m], "dp": lead - s}, rows.at[s, far[m], :, cut], slots.at[z, :, cut],
                        di_s.at[s], di_r.at[c],
                    ).start()
            if s == 0:
                slots[z, :, cut] = rows[s, z, :, cut]

        if relay:
            landed(hold.at[pl.ds(0, experts - 1)], su_r.at[1])
            for m in group_order:
                remote(
                    {"group": peer[m], "dp": 0}, hold, slots.at[:, :, subs[0]], su_s.at[1], su_r.at[2]
                ).start()

        compute(experts - 1, away, [])

        for s, c in turns(sets, len(back_cuts), 0, len(back_cuts) * lead):
            cut = back_cuts[c]
            landed(ret.at[s, pl.ds(0, experts if s else experts - 1), :, cut], re_r.at[c, s])
            both = dot(routes[s][1], ret[s, :, :, cut].reshape(experts * cap, cut.size))
            total = (both[: groups * own] + both[groups * own :]).astype(jnp.bfloat16)
            mixed[s, :, :, cut] = total.reshape(groups, own, cut.size)
            for m in group_order:
                if (s, m) != (lead, 0):
                    remote(
                        {"group": peer[m], "dp": s}, mixed.at[s, peer[m], :, cut], red.at[g, :, cut],
                        sc_s.at[s], sc_r.at[c],
                    ).start()
            if s == lead:
                pltpu.make_async_copy(mixed.at[s, g, :, cut], red.at[g, :, cut], sc_r.at[c]).start()

        if relay:
            landed(row_sub.at[pl.ds(0, experts - 1)], su_s.at[0])
            landed(rows.at[lead, :, :, pl.ds(0, skipped)], su_s.at[1])
        landed(tok.at[lead, pl.ds(0, groups - 1), :, pl.ds(0, width - skipped + sub)], ga_s)
        landed(part.at[pl.ds(0, experts - 1)], re_s)
        for s in range(sets):
            kept = width - skipped if s == lead else width
            landed(rows.at[s, pl.ds(0, experts if s else experts - 1), :, pl.ds(0, kept)], di_s.at[s])
            landed(mixed.at[s, pl.ds(0, groups - 1 if s == lead else groups)], sc_s.at[s])

    @pl.when(d != lead)
    def _():
        greet(dp=lead)
        for m in range(1, experts):
            greet(expert=far[m])
        load()
        tok_in.wait()
        named_in.wait()
        pl.semaphore_wait(go, 1)
        send_tokens(cuts, group_order)
        remote({"dp": lead}, named.at[d], named.at[d], id_s, id_r.at[d]).start()
        pl.semaphore_wait(barrier, 2 * (experts - 1))
        pl.semaphore_signal(go, inc=1, device_id={"dp": lead}, device_id_type=MESH)

        compute(experts, away[:URGENT] + [z], away[URGENT:])

        landed(tok.at[d], ga_s)
        landed(named.at[d], id_s)
        landed(part, re_s)

    for c, cut in enumerate(back_cuts):
        landed(red.at[:, :, cut], sc_r.at[c])
        total = red[0, :, cut].astype(jnp.float32)
        for k in range(1, groups):
            total = total + red[k, :, cut].astype(jnp.float32)
        out[:, cut] = total.astype(out.dtype)


def per_device(tokens, expert_ids, gate_codes, w_gate, w_up, w_down):
    groups = lax.axis_size("group")
    experts = lax.axis_size("expert")
    sets = lax.axis_size("dp")
    own, width = tokens.shape[1:]
    hid = w_gate.shape[2]
    bf16 = jnp.bfloat16
    sub = max(128, relayed(width, groups) // groups)
    any_space = pl.BlockSpec(memory_space=pl.ANY)
    dma = pltpu.SemaphoreType.DMA
    return pl.pallas_call(
        functools.partial(kernel, groups, experts, sets),
        out_shape=pltpu.VMEM((own, width), bf16),
        in_specs=[any_space] * 6,
        out_specs=pl.BlockSpec(memory_space=pltpu.VMEM),
        scratch_shapes=[
            pltpu.VMEM((groups, own, width), bf16),
            pltpu.VMEM((sets, groups, own, width), bf16),
            pltpu.VMEM((groups, own, sub), bf16),
            pltpu.VMEM((sets, 2, *expert_ids.shape[:0:-1]), jnp.int32),
            pltpu.VMEM((2, width, hid), bf16),
            pltpu.VMEM((hid, width), bf16),
            pltpu.VMEM((sets, experts, CAPG, width), bf16),
            pltpu.VMEM((experts, CAPG, sub), bf16),
            pltpu.VMEM((experts, CAPG, sub), bf16),
            pltpu.VMEM((experts, CAPG, width), bf16),
            pltpu.VMEM((2, experts * CAPG, hid), jnp.float32),
            pltpu.VMEM((experts, CAPG, width), bf16),
            pltpu.VMEM((sets, experts, CAPG, width), bf16),
            pltpu.VMEM((sets, groups, own, width), bf16),
            dma,
            dma,
            dma,
            dma,
            dma,
            dma((sets - 1,)),
            dma,
            dma((len(FORWARD), sets)),
            dma((sets,)),
            dma((len(FORWARD),)),
            dma,
            dma((len(BACK), sets)),
            dma((sets,)),
            dma((len(BACK),)),
            dma((2,)),
            dma((3,)),
            pltpu.SemaphoreType.REGULAR,
        ],
        compiler_params=pltpu.CompilerParams(
            collective_id=0, has_side_effects=True, vmem_limit_bytes=60 * 1024 * 1024
        ),
    )(tokens[0], expert_ids[0].T, gate_codes[0].T, w_gate[0], w_up[0], w_down[0])[None]


def solution(mesh):
    placed = (
        P(("expert", "dp"), "group", None),
        P(("expert", "dp"), None, None),
        P(("expert", "dp"), None, None),
        P("expert", None, "group"),
        P("expert", None, "group"),
        P("expert", "group", None),
    )
    return jax.shard_map(
        per_device,
        mesh=mesh,
        in_specs=placed,
        out_specs=P(("expert", "dp"), "group", None),
        check_vma=False,
    )
```
